32 devices in a mesh: groups: 2 (over y), expert: 4 (over z), tensor: 4 (over x, core).
Axes of the slice: x: 2, y: 2, z: 4, core: 2. Of those that a mesh axis runs over, the one named last changes fastest.
Arguments:
- tokens: bfloat16 [256, 4096], P(('groups', 'expert')), parts along dimension 0, may hold values from -6 to 6
- route_ids: int32 [256, 2], P(('groups', 'expert')), parts along dimension 0, may hold values from 0 to 3, all different within a row; in each aligned block of 32 rows (0 to 31, 32 to 63, ...) at most 24 rows name the same one
- route_gates: float32 [256, 2], P(('groups', 'expert')), parts along dimension 0, may hold values from 0.1 to 1
- gate_weight: bfloat16 [4096, 32768], P(None, ('expert', 'tensor')), may hold values from -0.09375 to 0.09375
- up_weight: bfloat16 [4096, 32768], P(None, ('expert', 'tensor')), may hold values from -0.09375 to 0.09375
- down_weight: bfloat16 [32768, 4096], P('expert', 'tensor'), may hold values from -0.0625 to 0.0625
Outputs:
- mixed: bfloat16 [256, 4096], P(('groups', 'expert'), 'tensor'), parts along dimension 0
The draws below stay inside these ranges and needn't reach their ends.
There are 2 independent parts, one for each index of `groups`. The reference program is written for one: setup_inputs(seed, part) draws one part's arguments, and reference() takes and returns one part's arrays. A program takes and returns all parts, laid end to end along the dimension named above; an argument that names none is the same for every part. Nothing has to cross between parts.
Inputs may be any that keep to these rules, and one draw needn't show every extreme that they name: `route_ids`: each row names 2 different experts. In the rows of one device no expert is named more than 24 times, and in some device's rows one expert is named exactly 24 times.
All inputs are finite; a program needn't handle non-finite values.
Results may differ from the reference program's by a relative error of at most 0.005.
Values may be sent and summed in bfloat16 or wider, within the bound.
A program may use at most 128 MiB of HBM per device.

```python
import math
import jax
import jax.numpy as jnp
import numpy as np
from jax import lax

D = 4096
FF = 8192
EXPERTS = 4
TOP = 2
TOK_DEV = 32
CAP = 24
TOKENS = 128


def levels(rng, shape, shards, least, high):
    gain = 1.0
    for axis_at, parts in shards:
        steps = jax.random.uniform(jax.random.fold_in(jax.random.fold_in(rng, 6), axis_at), (parts,), jnp.float32, least / len(shards), high / len(shards))
        gain = gain * jnp.repeat(jnp.exp(steps), shape[axis_at] // parts).reshape((-1,) + (1,) * (len(shape) - 1 - axis_at))
    return gain


def deal_out(rng, own, number, rows, number_of, top, limit, slope):
    ranking = jax.random.permutation(rng, number_of)
    crowded, ordinary = portions_of(number_of, rows * top, limit, slope, True), portions_of(number_of, rows * top, limit, slope, False)
    places = jnp.arange(number_of)

    def named(sizes, offset_by):
        used = int((sizes > 0).sum())
        fixed = max(1, used // 4)
        passed = fixed + (places - fixed + offset_by * (used - fixed)) % max(1, number_of - fixed)
        return jnp.zeros((number_of,), jnp.int32).at[ranking[jnp.where(places < fixed, places, passed)]].set(jnp.asarray(sizes, jnp.int32))

    sizes = jnp.where(number % 4 == 0, named(crowded, number // 4), named(ordinary, number - number // 4 - 1))
    mixed = jax.random.permutation(jax.random.fold_in(own, 3), number_of)
    giver, sink = mixed[0:number_of // 2 * 2:2], mixed[1:number_of // 2 * 2:2]
    slack = jnp.minimum(sizes[giver] - 1, limit - sizes[sink]) // 2
    slack = jnp.where((giver == ranking[0]) | (sink == ranking[0]) | (sizes[sink] == 0), 0, jnp.maximum(slack, 0))
    passed = jax.random.randint(jax.random.fold_in(own, 4), (number_of // 2,), 0, 1 << 20) % (slack + 1)
    sizes = sizes.at[giver].add(-passed).at[sink].add(passed)
    items = jnp.searchsorted(jnp.cumsum(sizes), jnp.arange(rows * top), side="right").astype(jnp.int32)
    grid = items.reshape(top, rows).T
    grid = grid[jax.random.permutation(jax.random.fold_in(own, 1), rows)]
    offset_by = jax.random.randint(jax.random.fold_in(own, 2), (rows, 1), 0, top)
    return jnp.take_along_axis(grid, (jnp.arange(top)[None, :] + offset_by) % top, axis=1)


def portions_of(amount, total, bound, slope, full):
    portions = [(1 << 20) // math.isqrt(rank ** slope) + 1 for rank in range(1, amount + 1)]
    largest = bound if full else min(bound, max(-(-total // amount), total * portions[0] // sum(portions)))
    least = 1 if total - largest >= amount - 1 else 0
    holding, surplus = [largest] + [least] * (amount - 1), total - largest - least * (amount - 1)
    while surplus > 0:
        free = [i for i in range(1, amount) if holding[i] < largest] or [i for i in range(1, amount) if holding[i] < bound]
        pool, remaining = sum([portions[i] for i in free]), surplus
        for i in free:
            extra = min(bound - holding[i], max(1, remaining * portions[i] // pool), surplus)
            holding[i] = holding[i] + extra
            surplus = surplus - extra
    return np.array(holding)


def noise(stream_key, shape, deviation, reach, cuts=(), kind=jnp.bfloat16):
    factor_of = levels(stream_key, shape, cuts, -0.22, 0.18) if cuts else 1.0
    result = jax.random.normal(stream_key, shape, jnp.float32) * deviation * factor_of
    return jnp.minimum(jnp.maximum(result, -reach), reach).astype(kind)


def setup_inputs(seed: int = 0, part: int = 0) -> dict:
    streams_of = jax.random.split(jax.random.key(seed), 7)
    part_splits = jax.random.split(jax.random.fold_in(streams_of[6], part), 7)
    tokens = noise(part_splits[0], (TOKENS, D), 1.0, 6.0, ((0, 4),))
    route_ids_keys = jax.random.split(jax.random.fold_in(part_splits[1], 1), TOKENS // TOK_DEV)
    route_ids_turns = jax.random.permutation(jax.random.fold_in(part_splits[1], 3), TOKENS // TOK_DEV)
    route_ids = jax.vmap(lambda own, number: deal_out(jax.random.fold_in(part_splits[1], 2), own, number, TOK_DEV, EXPERTS, TOP, CAP, 2))(route_ids_keys, route_ids_turns).reshape((TOKENS, TOP))
    route_gates = jnp.clip(jnp.exp(math.log(1.0) - 2.3025851 * jax.random.uniform(part_splits[2], (TOKENS, TOP), jnp.float32) ** levels(part_splits[2], (TOKENS, TOP), ((0, 4),), -0.2, 0.2)), 0.1, 1.0)
    gate_weight = noise(streams_of[3], (D, EXPERTS * FF), D ** -0.5, 0.09375, ((1, 16),))
    up_weight = noise(streams_of[4], (D, EXPERTS * FF), D ** -0.5, 0.09375, ((1, 16),))
    down_weight = noise(streams_of[5], (EXPERTS * FF, D), FF ** -0.5, 0.0625, ((0, 4), (1, 4)))
    return {"tokens": tokens, "route_ids": route_ids, "route_gates": route_gates, "gate_weight": gate_weight, "up_weight": up_weight, "down_weight": down_weight}


def reference(tokens, route_ids, route_gates, gate_weight, up_weight, down_weight):
    floats = tokens.astype(jnp.float32)
    scale = lax.rsqrt(lax.optimization_barrier(jnp.mean(floats * floats, axis=-1, keepdims=True)) + 1e-05)
    normed = (floats * scale).astype(jnp.bfloat16)

    def per_expert(total, expert):
        start = expert * FF
        gate_cols = lax.dynamic_slice_in_dim(gate_weight, start, FF, 1)
        up_cols = lax.dynamic_slice_in_dim(up_weight, start, FF, 1)
        down_rows = lax.dynamic_slice_in_dim(down_weight, start, FF, 0)
        gate_sum = jnp.dot(normed, gate_cols, preferred_element_type=jnp.float32)
        up_sum = jnp.dot(normed, up_cols, preferred_element_type=jnp.float32)
        hidden = (jax.nn.silu(gate_sum) * up_sum).astype(jnp.bfloat16)
        produced = jnp.dot(hidden, down_rows, preferred_element_type=jnp.float32)
        weight = lax.optimization_barrier(jnp.sum(jnp.where(route_ids == expert, route_gates, 0.0), axis=1))
        return (total + produced * weight[:, None], None)
    mixture, unused = lax.scan(per_expert, jnp.zeros((TOKENS, D), jnp.float32), jnp.arange(EXPERTS, dtype=jnp.int32))
    return (floats + mixture).astype(jnp.bfloat16)
```

```python
import functools

import jax
import jax.numpy as jnp
from jax import lax
from jax.experimental import pallas as pl
from jax.experimental.pallas import tpu as pltpu
from jax.sharding import PartitionSpec as P

EXPERTS = 4
CAP = 24
EPSILON = 1e-05
LAG = 4
MESH = pl.DeviceIdType.MESH
F32 = jnp.float32
BF16 = jnp.bfloat16


def kernel(
    n_e, n_t, chunks,
    tok_hbm, ids_hbm, gates_hbm, wg_hbm, wu_hbm, wd_hbm, out_ref,
    tok, ids, gates, normed, pick_t, combine, pack, recv, xs, wg, wu, wd, hid, acc, back, ret,
    small_sem, wg_sem, wu_sem, wd_sem,
    p1_send, p1_recv, p2x_send, p2c_send, p3_send, p2_recv,
    hx_send, hc_send, h3_send, h_recv, r_send, r_recv,
):
    e = lax.axis_index("expert")
    t = lax.axis_index("tensor")
    n_x = n_t // 2
    xi, core = t // 2, t % 2
    mate = xi * 2 + 1 - core
    blocks = n_e // EXPERTS
    rows, width = tok.shape
    sw = width // n_t
    served = n_e * CAP
    cw = hid.shape[3]
    hidden = wd.shape[0]

    def xpeer(d):
        return lax.rem(xi + d, n_x) * 2 + core

    def xmate(d):
        return lax.rem(xi + d, n_x) * 2 + 1 - core

    hops = sorted(range(1, n_e), key=lambda d: (abs(2 * d - n_e), d))
    far = list(range(1, n_x))

    smalls = [
        pltpu.make_async_copy(tok_hbm, tok, small_sem.at[0]),
        pltpu.make_async_copy(ids_hbm, ids, small_sem.at[1]),
        pltpu.make_async_copy(gates_hbm, gates, small_sem.at[2]),
    ]
    for c in smalls:
        c.start()

    barrier = pltpu.get_barrier_semaphore()
    for d in hops:
        pl.semaphore_signal(barrier, inc=1, device_id={"expert": lax.rem(e + d, n_e)}, device_id_type=MESH)
    for d in far:
        pl.semaphore_signal(barrier, inc=1, device_id={"tensor": xpeer(d)}, device_id_type=MESH)
    pl.semaphore_signal(barrier, inc=1, device_id={"tensor": mate}, device_id_type=MESH)

    def weight_copies(k):
        cols = pl.ds(k * cw, cw)
        return (
            pltpu.make_async_copy(wg_hbm.at[:, cols], wg.at[k], wg_sem.at[k]),
            pltpu.make_async_copy(wu_hbm.at[:, cols], wu.at[k], wu_sem.at[k]),
        )

    for k in range(chunks):
        for c in weight_copies(k):
            c.start()
    part = hidden // n_t
    downs = [
        pltpu.make_async_copy(wd_hbm.at[pl.ds(s * part, part)], wd.at[pl.ds(s * part, part)], wd_sem.at[s])
        for s in range(n_t)
    ]
    for c in downs:
        c.start()

    for c in smalls:
        c.wait()
    floats = tok[...].astype(F32)
    scale = lax.rsqrt(jnp.mean(floats * floats, axis=-1, keepdims=True) + EPSILON)
    normed[...] = (floats * scale).astype(BF16)
    slots = EXPERTS * CAP
    row = lax.broadcasted_iota(jnp.int32, (slots, rows), 0)
    of = jnp.zeros((slots, rows), jnp.int32)
    for x in range(1, EXPERTS):
        of = of + (row >= x * CAP).astype(jnp.int32)
    at = row - of * CAP
    named = [(ids[k : k + 1, :] == of).astype(F32) for k in range(ids.shape[0])]
    mask = functools.reduce(jnp.add, named)
    above = (
        lax.broadcasted_iota(jnp.int32, (rows, rows), 0) < lax.broadcasted_iota(jnp.int32, (rows, rows), 1)
    ).astype(F32)
    position = jnp.dot(mask.astype(BF16), above.astype(BF16), preferred_element_type=F32)
    hit = (position == at.astype(F32)).astype(F32)
    pick_t[...] = mask * hit
    mine = pl.ds(pl.multiple_of(t * sw, 128), sw)
    packed = jnp.dot(pick_t[...].astype(BF16), normed[:, mine], preferred_element_type=F32)
    for x in range(EXPERTS):
        pack[x] = packed[x * CAP : (x + 1) * CAP].astype(BF16)

    pl.semaphore_wait(barrier, len(hops) + len(far) + 1)

    def p1(src_e, dst_e, source):
        return pltpu.make_async_remote_copy(
            src_ref=pack.at[dst_e // blocks], dst_ref=recv.at[t, source],
            send_sem=p1_send.at[dst_e], recv_sem=p1_recv.at[source],
            device_id={"expert": dst_e}, device_id_type=MESH,
        )

    for d in hops:
        p1(e, lax.rem(e + d, n_e), e).start()

    weight = functools.reduce(jnp.add, [named[k] * gates[k : k + 1, :] for k in range(ids.shape[0])])
    combine[...] = (weight * hit).T
    own = pick_t[pl.ds(pl.multiple_of((e // blocks) * CAP, 8), CAP), :].astype(BF16)
    for s in range(n_t):
        recv[s, e] = jnp.dot(own, normed[:, s * sw : (s + 1) * sw], preferred_element_type=F32).astype(BF16)

    def move(ref, sends, recvs, send_at, slot, target):
        return pltpu.make_async_remote_copy(
            src_ref=ref.at[slot], dst_ref=ref.at[slot],
            send_sem=sends.at[send_at], recv_sem=recvs.at[slot],
            device_id={"tensor": target}, device_id_type=MESH,
        )

    sources = [lax.rem(e + n_e - d, n_e) for d in hops]
    for j in sources:
        p1(j, j, j).wait_recv()
        for d in far:
            move(recv, p2x_send, p2_recv, (d, j), (t, j), xpeer(d)).start()
        move(recv, p2c_send, p2_recv, j, (t, j), mate).start()
    def fill(s):
        flat = recv[s].astype(F32).reshape(served, sw).astype(BF16)
        xs[:, pl.ds(pl.multiple_of(s * sw, 128), sw)] = flat

    fill(t)
    for j in sources:
        for d in far:
            move(recv, p3_send, p2_recv, (d, j), (xpeer(d), j), mate).wait_recv()
            move(recv, p3_send, p2_recv, (d, j), (xpeer(d), j), mate).start()
    for d in far:
        fill(xpeer(d))
    for j in sources:
        move(recv, p2c_send, p2_recv, j, (mate, j), mate).wait_recv()
    fill(mate)
    for d in far:
        for j in sources:
            move(recv, p3_send, p2_recv, (d, j), (xmate(d), j), mate).wait_recv()
        fill(xmate(d))

    def relay(k):
        for d in far:
            c = move(hid, h3_send, h_recv, (d, k), (xpeer(d), k), mate)
            c.wait_recv()
            c.start()

    def gate_up(k):
        for c in weight_copies(k):
            c.wait()
        g = jnp.dot(xs[...], wg[k], preferred_element_type=F32)
        u = jnp.dot(xs[...], wu[k], preferred_element_type=F32)
        hid[t, k] = (g / (1.0 + jnp.exp(-g)) * u).astype(BF16)
        for d in far:
            move(hid, hx_send, h_recv, (d, k), (t, k), xpeer(d)).start()
        move(hid, hc_send, h_recv, k, (t, k), mate).start()

    for k in range(chunks):
        gate_up(k)
        if k >= LAG:
            relay(k - LAG)
    for c in downs:
        c.wait()

    def down(s, ks):
        total = None
        for k in ks:
            at_row = pl.ds(pl.multiple_of((s * chunks + k) * cw, 128), cw)
            part = jnp.dot(hid[s, k], wd[at_row, :], preferred_element_type=F32)
            total = part if total is None else total + part
        return total

    def from_mate(slot_of, ks):
        for k in ks:
            move(hid, hc_send, h_recv, k, (slot_of, k), mate).wait_recv()

    every = list(range(chunks))
    acc[...] = down(t, every)
    late = every[max(0, chunks - LAG) :]
    for i, k in enumerate(late):
        relay(k)
        if i == 0:
            from_mate(mate, every)
            acc[...] += down(mate, every)
    half = max(1, chunks // 2)
    for d in far:
        acc[...] += down(xpeer(d), every)
    for d in far:
        for ks in (every[:half], every[half:]):
            if ks:
                from_mate(xmate(d), ks)
                acc[...] += down(xmate(d), ks)

    for j in range(n_e):
        back[j] = acc[j * CAP : (j + 1) * CAP, :].astype(BF16)

    def giving(dst_e, source):
        return pltpu.make_async_remote_copy(
            src_ref=back.at[dst_e], dst_ref=ret.at[source],
            send_sem=r_send.at[dst_e], recv_sem=r_recv.at[source],
            device_id={"expert": dst_e}, device_id_type=MESH,
        )

    for d in hops:
        giving(lax.rem(e + d, n_e), e).start()
    ret[e] = back[e]

    for d in hops:
        p1(e, lax.rem(e + d, n_e), e).wait_send()
    for j in sources:
        for d in far:
            move(recv, p2x_send, p2_recv, (d, j), (t, j), xpeer(d)).wait_send()
            move(recv, p3_send, p2_recv, (d, j), (xpeer(d), j), mate).wait_send()
        move(recv, p2c_send, p2_recv, j, (t, j), mate).wait_send()

    def drain(k, carry):
        for d in far:
            move(hid, hx_send, h_recv, (d, k), (t, k), xpeer(d)).wait_send()
            move(hid, h3_send, h_recv, (d, k), (xpeer(d), k), mate).wait_send()
        move(hid, hc_send, h_recv, k, (t, k), mate).wait_send()
        return carry

    lax.fori_loop(0, chunks, drain, 0)

    for j in sources:
        giving(j, j).wait_recv()
    parts = []
    for x in range(EXPERTS):
        total = ret[x * blocks].astype(F32)
        for b in range(1, blocks):
            total = total + ret[x * blocks + b].astype(F32)
        parts.append(total)
    mixture = jnp.dot(
        combine[...], jnp.concatenate(parts, axis=0),
        precision=lax.Precision.HIGHEST, preferred_element_type=F32,
    )
    out_ref[...] = (tok[:, mine].astype(F32) + mixture).astype(BF16)
    for d in hops:
        giving(lax.rem(e + d, n_e), e).wait_send()


def solution(mesh):
    n_e, n_t = mesh.shape["expert"], mesh.shape["tensor"]

    def local(tokens, route_ids, route_gates, gate_weight, up_weight, down_weight):
        rows, width = tokens.shape
        own_hidden = gate_weight.shape[1]
        hidden, out_w = down_weight.shape
        sw = width // n_t
        cw = min(256, own_hidden)
        chunks = own_hidden // cw
        served = n_e * CAP
        dma = pltpu.SemaphoreType.DMA
        n_x = n_t // 2
        scratch = [
            pltpu.VMEM((rows, width), BF16),
            pltpu.VMEM(route_ids.shape[::-1], jnp.int32),
            pltpu.VMEM(route_gates.shape[::-1], F32),
            pltpu.VMEM((rows, width), BF16),
            pltpu.VMEM((EXPERTS * CAP, rows), F32),
            pltpu.VMEM((rows, EXPERTS * CAP), F32),
            pltpu.VMEM((EXPERTS, CAP, sw), BF16),
            pltpu.VMEM((n_t, n_e, CAP, sw), BF16),
            pltpu.VMEM((served, width), BF16),
            pltpu.VMEM((chunks, width, cw), BF16),
            pltpu.VMEM((chunks, width, cw), BF16),
            pltpu.VMEM((hidden, out_w), BF16),
            pltpu.VMEM((n_t, chunks, served, cw), BF16),
            pltpu.VMEM((served, out_w), F32),
            pltpu.VMEM((n_e, CAP, out_w), BF16),
            pltpu.VMEM((n_e, CAP, out_w), BF16),
            dma((3,)), dma((chunks,)), dma((chunks,)), dma((n_t,)),
            dma((n_e,)), dma((n_e,)), dma((n_x, n_e)), dma((n_e,)), dma((n_x, n_e)), dma((n_t, n_e)),
            dma((n_x, chunks)), dma((chunks,)), dma((n_x, chunks)), dma((n_t, chunks)), dma((n_e,)), dma((n_e,)),
        ]
        return pl.pallas_call(
            functools.partial(kernel, n_e, n_t, chunks),
            out_shape=jax.ShapeDtypeStruct((rows, out_w), BF16),
            in_specs=[pl.BlockSpec(memory_space=pl.ANY)] * 6,
            out_specs=pl.BlockSpec(memory_space=pltpu.VMEM),
            scratch_shapes=scratch,
            compiler_params=pltpu.CompilerParams(
                collective_id=0, has_side_effects=True, vmem_limit_bytes=57_000_000
            ),
        )(tokens, route_ids.T, route_gates.T, gate_weight, up_weight, down_weight)

    in_specs = (
        P(("groups", "expert"), None),
        P(("groups", "expert"), None),
        P(("groups", "expert"), None),
        P(None, ("expert", "tensor")),
        P(None, ("expert", "tensor")),
        P("expert", "tensor"),
    )
    return jax.shard_map(
        local, mesh=mesh, in_specs=in_specs, out_specs=P(("groups", "expert"), "tensor"), check_vma=False
    )
```
